256 devices in a mesh: cuts: 4 (over y, x), wide: 32 (over z), batch: 2 (over core).
Axes of the slice: x: 2, y: 2, z: 32, core: 2. Of those that a mesh axis runs over, the one named last changes fastest.
The devices are a block of a 4x8x32 slice.
Arguments:
- initial: bfloat16 [2, 128, 2, 2, 256, 256], P('batch', 'cuts', None, None, None, 'wide'), parts along dimension 1, may hold values from -6 to 6
- branches: bfloat16 [8, 2, 2, 256, 2, 256], P(None, None, None, 'batch'), may hold values from -0.1875 to 0.1875
- projectors: float32 [8, 2, 2, 2], replicated, may hold values from -4 to 4
- bits: int32 [2, 8], P('batch'), may hold values from 0 to 1
Outputs:
- amplitudes: float32 [2, 128, 2, 2, 256, 256], P('batch', 'cuts', None, None, 'wide'), parts along dimension 1
The draws below stay inside these ranges and needn't reach their ends.
There are 4 independent parts, one for each index of `cuts`. The reference program is written for one: setup_inputs(seed, part) draws one part's arguments, and reference() takes and returns one part's arrays. A program takes and returns all parts, laid end to end along the dimension named above; an argument that names none is the same for every part. Nothing has to cross between parts.
Inputs may be any that keep to these rules, and one draw needn't show every extreme that they name: `bits`: each entry is a bit.
All inputs are finite; a program needn't handle non-finite values.
Results may differ from the reference program's by a relative error of at most 0.014.
Values may be sent and summed in bfloat16 or wider, within the bound.
No kernel may reach another device: no remote copies, remote signals or barrier semaphores. Data moves between devices by JAX's collectives and lax.ppermute only.
A program may use at most 64 MiB of HBM per device.

```python
import jax
import jax.numpy as jnp

QGROUP = 256
HSHARED = 2
COLUMNS = 32
STEPS = 8
BATCH = 2


def set_ends(values, own_key, least, largest):
    dims = values.shape
    place = [jax.random.randint(jax.random.fold_in(own_key, axis), (), 0, dims[axis]) for axis in range(len(dims))]
    values = values.at[tuple(place)].set(least)
    longest = dims.index(max(dims))
    place[longest] = (place[longest] + 1) % dims[longest]
    return values.at[tuple(place)].set(largest)


def level_of(rng, extent, split, smallest, top_value):
    factor_of, own = 1.0, jax.random.fold_in(rng, 6)
    for dim, shards_of in split:
        steps = jnp.exp(jax.random.uniform(jax.random.fold_in(own, dim), (shards_of,), jnp.float32, smallest / len(split), top_value / len(split)))
        factor_of = factor_of * jnp.repeat(steps, extent[dim] // shards_of).reshape([-1 if axis == dim else 1 for axis in range(len(extent))])
    return factor_of


def scatter_about(rng, dims, deviation, limit, pieces=(), kind=jnp.bfloat16):
    values = jax.random.normal(rng, dims, jnp.float32) * deviation
    if len(pieces) > 0:
        values = level_of(rng, dims, pieces, -0.22, 0.18) * values
    return jnp.clip(values, min=-limit, max=limit).astype(kind)


def setup_inputs(seed: int = 0, part: int = 0) -> dict:
    keys = jax.random.split(jax.random.key(seed), 5)
    part_keys = jax.random.split(jax.random.fold_in(keys[4], part), 5)
    initial = scatter_about(part_keys[0], (BATCH, COLUMNS, 2, HSHARED, QGROUP, QGROUP), 1.0, 6.0, ((0, 2), (5, 32)))
    branches = scatter_about(keys[1], (STEPS, 2, HSHARED, QGROUP, HSHARED, QGROUP), (2 * HSHARED * QGROUP) ** -0.5, 0.1875, ((3, 2),))
    projectors = scatter_about(keys[2], (STEPS, 2, 2, HSHARED), 0.7, 4.0, (), jnp.float32)
    bits = set_ends(jax.random.randint(keys[3], (BATCH, STEPS), 0, 2), jax.random.fold_in(keys[3], 1), 0, 1).astype(jnp.int32)
    return {"initial": initial, "branches": branches, "projectors": projectors, "bits": bits}


def contract(state, branch, select):
    prod = jnp.einsum('ncphuv,thugw->ncptgvw', state.astype(jnp.float32), branch.astype(jnp.float32))
    real_part = prod[:, :, 0, 0] - prod[:, :, 1, 1]
    imag_part = prod[:, :, 0, 1] + prod[:, :, 1, 0]
    proj_re = select[:, 0][:, None, :, None, None]
    proj_im = select[:, 1][:, None, :, None, None]
    out_re = proj_re * real_part - proj_im * imag_part
    out_im = proj_re * imag_part + proj_im * real_part
    return jnp.stack([out_re, out_im], axis=2)


def reference(initial, branches, projectors, bits):
    state = initial
    result = None
    for step in range(STEPS):
        chosen = (bits[:, step] == 1)[:, None, None]
        select = jnp.where(chosen, projectors[step, 1][None], projectors[step, 0][None])
        result = contract(state, branches[step], select)
        state = result.astype(jnp.bfloat16)
    return result
```

```python
import functools

import jax
import jax.numpy as jnp
from jax import lax
from jax.experimental import pallas as pl
from jax.experimental.pallas import tpu as pltpu
from jax.sharding import PartitionSpec as P


def factor(proj_ref, bits_ref, step, g):
    bit = jnp.where(bits_ref[0, step] == 1, 1, 0)
    return proj_ref[step, bit, 0, g], proj_ref[step, bit, 1, g]


def project(real, imag, scale):
    scale_re, scale_im = scale
    return scale_re * real - scale_im * imag, scale_re * imag + scale_im * real


def weight_copies(w_ref, x_ref, buf, sem, transposed):
    me = lax.axis_index("batch")
    half = w_ref.shape[-1] if transposed else w_ref.shape[-2]
    copies = []
    for ref, owner in ((w_ref, me), (x_ref, 1 - me)):
        start = pl.multiple_of(owner * half, half)
        if transposed:
            blocks = ref.shape[1]
            for b in range(blocks):
                at = pl.multiple_of(owner * half + b * 2 * half, half)
                copies.append(pltpu.make_async_copy(ref.at[:, b], buf.at[:, :, pl.ds(at, half)], sem))
        else:
            copies.append(pltpu.make_async_copy(ref, buf.at[:, :, pl.ds(start, half), :], sem))
    return copies


def by_rows(got_ref, form):
    n, blocks, rows, q = got_ref.shape
    h = blocks // 2
    for k in range(blocks):
        block = got_ref[:, k].reshape(n * rows, q)
        if k < h:
            form[:, pl.ds((h + k) * q, q)] = block
        else:
            form[:, pl.ds((k - h) * q, q)] = block
            form[:, pl.ds((h + k) * q, q)] = -block


NN = (((1,), (0,)), ((), ()))
NT = (((1,), (1,)), ((), ()))


def dot(a, b, dims):
    return lax.dot_general(a, b, dims, preferred_element_type=jnp.float32)


def chain_kernel(n_steps, q, hs, proj_ref, bits_ref, got_ref, *refs):
    mine, other = refs[:n_steps], refs[n_steps : 2 * n_steps]
    out_ref = refs[2 * n_steps]
    bufs = refs[2 * n_steps + 1 : 3 * n_steps + 1]
    rows_form, cols_form, sems = refs[3 * n_steps + 1 :]
    last = n_steps - 1
    kinds = [s % 2 == 1 or s == last for s in range(n_steps)]
    copies = [weight_copies(mine[s], other[s], bufs[s], sems.at[s], kinds[s]) for s in range(n_steps)]
    for step in copies:
        for copy in step:
            copy.start()
    by_rows(got_ref, rows_form)
    k = 2 * hs * q
    for s in range(n_steps):
        for copy in copies[s]:
            copy.wait()
        for g in range(hs):
            scale = factor(proj_ref, bits_ref, s, g)
            if s == last:
                w = bufs[s][g]
                real = dot(w, rows_form[:, pl.ds(hs * q, k)], NT)
                imag = dot(w, rows_form[:, pl.ds(0, k)], NT)
                real, imag = project(real, imag, scale)
                n, _, part, _ = out_ref.shape
                out_ref[:, g] = real.astype(out_ref.dtype).reshape(n, part, q)
                out_ref[:, hs + g] = imag.astype(out_ref.dtype).reshape(n, part, q)
            elif s % 2 == 0:
                w = bufs[s][g].reshape(k, q)
                real = dot(rows_form[:, pl.ds(hs * q, k)], w, NN)
                imag = dot(rows_form[:, pl.ds(0, k)], w, NN)
                real, imag = project(real, imag, scale)
                imag = imag.astype(cols_form.dtype)
                cols_form[pl.ds((hs + g) * q, q), :] = real.astype(cols_form.dtype)
                cols_form[pl.ds(g * q, q), :] = imag
                cols_form[pl.ds((2 * hs + g) * q, q), :] = -imag
            else:
                w = bufs[s][g]
                real = dot(w, cols_form[pl.ds(hs * q, k), :], NN)
                imag = dot(w, cols_form[pl.ds(0, k), :], NN)
                real, imag = project(real, imag, scale)
                imag = imag.astype(rows_form.dtype)
                rows_form[:, pl.ds((hs + g) * q, q)] = real.astype(rows_form.dtype)
                rows_form[:, pl.ds(g * q, q)] = imag
                rows_form[:, pl.ds((2 * hs + g) * q, q)] = -imag


def last_kernel(step, q, hs, proj_ref, bits_ref, got_ref, mine, other, out_ref, buf, rows_form, sem):
    copies = weight_copies(mine, other, buf, sem, False)
    for copy in copies:
        copy.start()
    by_rows(got_ref, rows_form)
    for copy in copies:
        copy.wait()
    k = 2 * hs * q
    n, _, _, part, _ = out_ref.shape
    for g in range(hs):
        w = buf[g].reshape(k, q)
        real = dot(rows_form[:, pl.ds(hs * q, k)], w, NN)
        imag = dot(rows_form[:, pl.ds(0, k)], w, NN)
        real, imag = project(real, imag, factor(proj_ref, bits_ref, step, g))
        out_ref[:, 0, g] = real.reshape(n, part, q)
        out_ref[:, 1, g] = imag.reshape(n, part, q)


SMEM = pl.BlockSpec(memory_space=pltpu.SMEM)
VMEM = pl.BlockSpec(memory_space=pltpu.VMEM)
ANY = pl.BlockSpec(memory_space=pl.ANY)


def laid_out(branches, step, transposed):
    b = branches[step]
    parts, hs, half, gs, q = b.shape
    if transposed:
        return b.transpose(3, 0, 1, 4, 2).reshape(gs, parts * hs, q, half)
    return b.transpose(3, 0, 1, 2, 4).reshape(gs, parts * hs, half, q)


def shards(initial, branches, projectors, bits):
    steps, parts, hs, half, _, q = branches.shape
    _, cols, _, _, _, part = initial.shape
    n_chain = steps - 1
    sent = jnp.swapaxes(initial, 4, 5).reshape(cols, parts * hs, part, q)
    swapped = lax.ppermute(branches, "batch", [(0, 1), (1, 0)])
    got = lax.all_to_all(sent, "wide", split_axis=0, concat_axis=0, tiled=True)
    kinds = [s % 2 == 1 or s == n_chain - 1 for s in range(n_chain)] + [False]
    mine = [laid_out(branches, s, kinds[s]) for s in range(steps)]
    other = [laid_out(swapped, s, kinds[s]) for s in range(steps)]
    bufs = [pltpu.VMEM((hs, q, parts * hs * q) if t else (hs, parts * hs, q, q), jnp.bfloat16) for t in kinds]
    flops = 2 * 2 * parts * hs * q * hs * q * q
    state = pl.pallas_call(
        functools.partial(chain_kernel, n_chain, q, hs),
        out_shape=jax.ShapeDtypeStruct((cols, parts * hs, part, q), jnp.bfloat16),
        in_specs=[SMEM, SMEM, VMEM] + [ANY] * (2 * n_chain),
        out_specs=VMEM,
        scratch_shapes=bufs[:n_chain]
        + [
            pltpu.VMEM((q, 3 * hs * q), jnp.bfloat16),
            pltpu.VMEM((3 * hs * q, q), jnp.bfloat16),
            pltpu.SemaphoreType.DMA((n_chain,)),
        ],
        compiler_params=pltpu.CompilerParams(vmem_limit_bytes=40 * 2**20),
        cost_estimate=pl.CostEstimate(flops=n_chain * flops, bytes_accessed=8 * 2**20, transcendentals=0),
        name="chain",
    )(projectors, bits, got, *mine[:n_chain], *other[:n_chain])
    back = lax.all_to_all(state, "wide", split_axis=0, concat_axis=0, tiled=True)
    out = pl.pallas_call(
        functools.partial(last_kernel, n_chain, q, hs),
        out_shape=jax.ShapeDtypeStruct((cols, parts, hs, part, q), jnp.float32),
        in_specs=[SMEM, SMEM, VMEM, ANY, ANY],
        out_specs=VMEM,
        scratch_shapes=[bufs[n_chain], pltpu.VMEM((q, 3 * hs * q), jnp.bfloat16), pltpu.SemaphoreType.DMA],
        compiler_params=pltpu.CompilerParams(vmem_limit_bytes=40 * 2**20),
        cost_estimate=pl.CostEstimate(flops=flops, bytes_accessed=3 * 2**20, transcendentals=0),
        name="last",
    )(projectors, bits, back, mine[n_chain], other[n_chain])
    return out[None]


def solution(mesh):
    in_specs = (
        P("batch", "cuts", None, None, None, "wide"),
        P(None, None, None, "batch", None, None),
        P(),
        P("batch", None),
    )
    out_specs = P("batch", "cuts", None, None, "wide", None)
    return jax.shard_map(shards, mesh=mesh, in_specs=in_specs, out_specs=out_specs, check_vma=False)
```
